32 devices in a mesh: groups: 2 (over y), expert: 8 (over z, core), tensor: 2 (over x).
Axes of the slice: x: 2, y: 2, z: 4, core: 2. Of those that a mesh axis runs over, the one named last changes fastest.
Arguments:
- hidden_in: bfloat16 [128, 2880], P(('groups', 'expert')), parts along dimension 0, may hold values from -6 to 6
- queries: bfloat16 [128, 32, 64], P(('groups', 'expert'), 'tensor'), parts along dimension 0, may hold values from -8 to 8
- new_keys: bfloat16 [128, 8, 64], P(('groups', 'expert'), 'tensor'), parts along dimension 0, may hold values from -4 to 4
- new_values: bfloat16 [128, 8, 64], P(('groups', 'expert'), 'tensor'), parts along dimension 0, may hold values from -4 to 4
- cache_keys: bfloat16 [128, 8, 64, 256], P(('groups', 'expert'), 'tensor'), parts along dimension 0, may hold values from -8 to 8
- cache_values: bfloat16 [128, 8, 64, 256], P(('groups', 'expert'), 'tensor'), parts along dimension 0, may hold values from -4 to 4
- cache_lengths: int32 [128], P(('groups', 'expert')), parts along dimension 0, may hold values from 2 to 256, as said below
- out_weight: bfloat16 [2048, 2880], P('tensor'), may hold values from -0.125 to 0.125
- norm_gain: float32 [2880], replicated, may hold values from 0.1 to 1.9
- expert_ids: int32 [128, 4], P(('groups', 'expert')), parts along dimension 0, may hold values from 0 to 7, all different within a row; in each aligned block of 8 rows (0 to 7, 8 to 15, ...) at most 4 rows name the same one
- route_probs: float32 [128, 4], P(('groups', 'expert')), parts along dimension 0, may hold values from 0.05 to 1
- route_order: int32 [128, 4], P(('groups', 'expert')), parts along dimension 0, may hold values from 0 to 3, each once within a row
- gate_weight: bfloat16 [8, 2880, 1440], P('expert', None, 'tensor'), may hold values from -0.109375 to 0.109375
- up_weight: bfloat16 [8, 2880, 1440], P('expert', None, 'tensor'), may hold values from -0.109375 to 0.109375
- down_weight: bfloat16 [8, 1440, 2880], P('expert', 'tensor'), may hold values from -0.15625 to 0.15625
Outputs:
- layer_out: bfloat16 [128, 2880], P(('groups', 'expert'), 'tensor'), parts along dimension 0
The draws below stay inside these ranges and needn't reach their ends.
There are 2 independent parts, one for each index of `groups`. The reference program is written for one: setup_inputs(seed, part) draws one part's arguments, and reference() takes and returns one part's arrays. A program takes and returns all parts, laid end to end along the dimension named above; an argument that names none is the same for every part. Nothing has to cross between parts.
Inputs may be any that keep to these rules, and one draw needn't show every extreme that they name: `cache_lengths`: some sequence fills all 256 slots. `expert_ids`: each row names 4 different experts; among the 8 rows of one device no expert is named by more than 4 rows, a bound that some block reaches. `route_order`: each row is a permutation of 0 to 3.
All inputs are finite; a program needn't handle non-finite values.
Results may differ from the reference program's by a relative error of at most 0.007.
Values may be sent and summed in bfloat16 or wider, within the bound.
A program may use at most 64 MiB of HBM per device.

```python
import math
from functools import partial
import jax
import jax.numpy as jnp
import numpy as np
from jax import lax

D = 2880
FF = 1440
HEADS = 32
KVH = 8
HD = 64
TOP = 4
SEQ_DEV = 8
CACHE = 256
SEQS = 64
EXPERTS = 8
CAP = 4


def draw_queries(key, part):
    noise_key = jax.random.fold_in(key, 3)
    values = jnp.clip(jax.random.normal(noise_key, (SEQS, HEADS, HD), jnp.float32), -4.0, 4.0)
    return values.astype(jnp.bfloat16)


def draw_cache_keys(key, part):
    noise_key = jax.random.fold_in(key, 5)
    values = jnp.clip(jax.random.normal(noise_key, (SEQS, KVH, HD, CACHE), jnp.float32), -4.0, 4.0)
    return values.astype(jnp.bfloat16)


def draw_cache_lengths(key, part):
    length_key, pick_key = jax.random.split(jax.random.fold_in(key, 11))
    drawn_lengths = jax.random.randint(length_key, (SEQS,), 2, CACHE + 1)
    chosen = jax.random.randint(pick_key, (), 0, SEQS)
    return jnp.where(jnp.arange(SEQS) == chosen, CACHE, drawn_lengths).astype(jnp.int32)


def block_scale(own_key, shape, pieces, smallest, largest):
    level = 1.0
    for dim, shards_of in pieces:
        heights = jax.random.uniform(jax.random.fold_in(jax.random.fold_in(own_key, 6), dim), (shards_of,), jnp.float32, smallest / len(pieces), largest / len(pieces))
        level = level * jnp.repeat(jnp.exp(heights), shape[dim] // shards_of).reshape((-1,) + (1,) * (len(shape) - 1 - dim))
    return level


def routed_block(key, own, number, rows, number_of, top, most, slope):
    sequence = jax.random.permutation(key, number_of)
    packed, ordinary = shares(number_of, rows * top, most, slope, True), shares(number_of, rows * top, most, slope, False)
    places = jnp.arange(number_of)

    def named(lengths, offset_by):
        used = int((lengths > 0).sum())
        fixed = max(1, used // 4)
        passed = fixed + (places - fixed + offset_by * (used - fixed)) % max(1, number_of - fixed)
        return jnp.zeros((number_of,), jnp.int32).at[sequence[jnp.where(places < fixed, places, passed)]].set(jnp.asarray(lengths, jnp.int32))

    lengths = jnp.where(number % 4 == 0, named(packed, number // 4), named(ordinary, number - number // 4 - 1))
    mixed = jax.random.permutation(jax.random.fold_in(own, 3), number_of)
    source_of, receiver = mixed[0:number_of // 2 * 2:2], mixed[1:number_of // 2 * 2:2]
    slack = jnp.minimum(lengths[source_of] - 1, most - lengths[receiver]) // 2
    slack = jnp.where((source_of == sequence[0]) | (receiver == sequence[0]) | (lengths[receiver] == 0), 0, jnp.maximum(slack, 0))
    passed = jax.random.randint(jax.random.fold_in(own, 4), (number_of // 2,), 0, 1 << 20) % (slack + 1)
    lengths = lengths.at[source_of].add(-passed).at[receiver].add(passed)
    items = jnp.searchsorted(jnp.cumsum(lengths), jnp.arange(rows * top), side="right").astype(jnp.int32)
    listing = items.reshape(top, rows).T
    listing = listing[jax.random.permutation(jax.random.fold_in(own, 1), rows)]
    offset_by = jax.random.randint(jax.random.fold_in(own, 2), (rows, 1), 0, top)
    return jnp.take_along_axis(listing, (jnp.arange(top)[None, :] + offset_by) % top, axis=1)


def shares(amount, total, most, lean, full):
    weights = [(1 << 20) // math.isqrt(rank ** lean) + 1 for rank in range(1, amount + 1)]
    largest = most if full else min(most, max(-(-total // amount), total * weights[0] // sum(weights)))
    least = 1 if total - largest >= amount - 1 else 0
    counts, rest = [largest] + [least] * (amount - 1), total - largest - least * (amount - 1)
    while rest > 0:
        candidates = [i for i in range(1, amount) if counts[i] < largest] or [i for i in range(1, amount) if counts[i] < most]
        mass, remaining = sum([weights[i] for i in candidates]), rest
        for i in candidates:
            more = min(most - counts[i], max(1, remaining * weights[i] // mass), rest)
            counts[i] = counts[i] + more
            rest = rest - more
    return np.array(counts)


def gaussian(own_key, dims, spread, limit, shards=(), kind=jnp.bfloat16):
    result = jax.random.normal(own_key, dims, jnp.float32) * spread
    if len(shards) > 0:
        result = block_scale(own_key, dims, shards, -0.22, 0.18) * result
    return jnp.clip(result, min=-limit, max=limit).astype(kind)


def setup_inputs(seed: int = 0, part: int = 0) -> dict:
    keys = jax.random.split(jax.random.key(seed), 16)
    part_splits = jax.random.split(jax.random.fold_in(keys[15], part), 16)
    hidden_in = gaussian(part_splits[0], (SEQS, D), 1.0, 6.0, ((0, 8),))
    queries = draw_queries(jax.random.fold_in(jax.random.fold_in(keys[15], part), 71), part)
    new_keys = gaussian(part_splits[2], (SEQS, KVH, HD), 1.0, 4.0, ((0, 8), (1, 2)))
    new_values = gaussian(part_splits[3], (SEQS, KVH, HD), 1.0, 4.0, ((0, 8), (1, 2)))
    cache_keys = draw_cache_keys(jax.random.fold_in(jax.random.fold_in(keys[15], part), 71), part)
    cache_values = gaussian(part_splits[5], (SEQS, KVH, HD, CACHE), 1.0, 4.0, ((0, 8), (1, 2)))
    cache_lengths = draw_cache_lengths(jax.random.fold_in(jax.random.fold_in(keys[15], part), 71), part)
    out_weight = gaussian(keys[7], (HEADS * HD, D), (HEADS * HD) ** -0.5, 0.125, ((0, 2),))
    norm_gain = jnp.clip(1.0 + 0.18 * jax.random.normal(keys[8], (D,), jnp.float32), 0.1, 1.9)
    expert_ids_keys = jax.random.split(jax.random.fold_in(part_splits[9], 1), SEQS // SEQ_DEV)
    expert_ids_turns = jax.random.permutation(jax.random.fold_in(part_splits[9], 3), SEQS // SEQ_DEV)
    expert_ids = jax.vmap(lambda own, number: routed_block(jax.random.fold_in(part_splits[9], 2), own, number, SEQ_DEV, EXPERTS, TOP, CAP, 2))(expert_ids_keys, expert_ids_turns).reshape((SEQS, TOP))
    route_probs = jnp.clip(jnp.exp(math.log(1.0) - 2.9957323 * jax.random.uniform(part_splits[10], (SEQS, TOP), jnp.float32) ** block_scale(part_splits[10], (SEQS, TOP), ((0, 8),), -0.2, 0.2)), 0.05, 1.0)
    route_order = jax.vmap(lambda own: jax.random.permutation(own, TOP))(jax.random.split(part_splits[11], SEQS)).reshape((SEQS, TOP)).astype(jnp.int32)
    gate_weight = gaussian(keys[12], (EXPERTS, D, FF), D ** -0.5, 0.109375, ((0, 8), (2, 2)))
    up_weight = gaussian(keys[13], (EXPERTS, D, FF), D ** -0.5, 0.109375, ((0, 8), (2, 2)))
    down_weight = gaussian(keys[14], (EXPERTS, FF, D), FF ** -0.5, 0.15625, ((0, 8), (1, 2)))
    return dict(hidden_in=hidden_in, queries=queries, new_keys=new_keys, new_values=new_values, cache_keys=cache_keys, cache_values=cache_values, cache_lengths=cache_lengths, out_weight=out_weight, norm_gain=norm_gain, expert_ids=expert_ids, route_probs=route_probs, route_order=route_order, gate_weight=gate_weight, up_weight=up_weight, down_weight=down_weight)


EPSILON = 1e-05
GLU_SLOPE = 1.702

def attend(queries, new_keys, new_values, cache_keys, cache_values, cache_lengths):
    sequence_count, head_count, head_dim = queries.shape
    kv_heads = new_keys.shape[1]
    group_size = head_count // kv_heads
    scaling = 1.0 / head_dim ** 0.5
    query_rows = queries.astype(jnp.float32).reshape(sequence_count, kv_heads, group_size, head_dim)
    scores = jnp.einsum('sgqd,sgdc->sgqc', query_rows, cache_keys.astype(jnp.float32)) * scaling
    own_score = jnp.einsum('sgqd,sgd->sgq', query_rows, new_keys.astype(jnp.float32)) * scaling
    positions = jnp.arange(cache_keys.shape[3], dtype=jnp.int32)
    visible = positions[None, :] < cache_lengths[:, None]
    scores = jnp.where(visible[:, None, None, :], scores, -1e+30)
    highest = jnp.maximum(lax.optimization_barrier(jnp.max(scores, axis=3)), own_score)
    cache_exp = jnp.exp(scores - highest[..., None])
    own_exp = jnp.exp(own_score - highest)
    totals = lax.optimization_barrier(jnp.sum(cache_exp, axis=3)) + own_exp
    cache_prob = (cache_exp / totals[..., None]).astype(jnp.bfloat16)
    own_prob = (own_exp / totals).astype(jnp.bfloat16)
    attended = jnp.einsum('sgqc,sgdc->sgqd', cache_prob.astype(jnp.float32), cache_values.astype(jnp.float32))
    attended = attended + own_prob.astype(jnp.float32)[..., None] * new_values.astype(jnp.float32)[:, :, None, :]
    return attended.astype(jnp.bfloat16).reshape(sequence_count, head_count * head_dim)

def apply_norm(residual, norm_gain):
    mean_square = lax.optimization_barrier(jnp.mean(residual * residual, axis=1, keepdims=True))
    return (residual * lax.rsqrt(mean_square + EPSILON) * norm_gain).astype(jnp.bfloat16)

def route_tables(expert_ids, route_probs, route_order, experts, capacity):
    tokens, top_count = expert_ids.shape
    flat_ids = expert_ids.reshape(tokens * top_count)
    expert_mark = (flat_ids[:, None] == jnp.arange(experts, dtype=jnp.int32)[None, :]).astype(jnp.int32)
    earlier = jnp.cumsum(expert_mark, axis=0) - expert_mark
    position = lax.optimization_barrier(jnp.sum(earlier * expert_mark, axis=1))
    slot_code = flat_ids * capacity + position
    slot_table = slot_code[:, None] == jnp.arange(experts * capacity, dtype=jnp.int32)[None, :]
    slot_table = slot_table.astype(jnp.float32).reshape(tokens, top_count, experts * capacity)
    picked = jnp.zeros((tokens, top_count), jnp.float32)
    for column in range(top_count):
        picked = picked + jnp.where(route_order == column, route_probs[:, column:column + 1], 0.0)
    weights = picked / lax.optimization_barrier(jnp.sum(route_probs, axis=1, keepdims=True))
    select_experts = lax.optimization_barrier(jnp.sum(slot_table, axis=1))
    weighted_output = lax.optimization_barrier(jnp.sum(slot_table * weights[:, :, None], axis=1))
    return (select_experts, weighted_output)

def expert_block(operands):
    token_rows, gate_part, up_part, down_part = operands
    gate_sums = jnp.dot(token_rows, gate_part, preferred_element_type=jnp.float32)
    upward = jnp.dot(token_rows, up_part, preferred_element_type=jnp.float32)
    active = (gate_sums * jax.nn.sigmoid(GLU_SLOPE * gate_sums) * (upward + 1.0)).astype(jnp.bfloat16)
    return jnp.dot(active, down_part, preferred_element_type=jnp.float32)

def reference(hidden_in, queries, new_keys, new_values, cache_keys, cache_values, cache_lengths, out_weight, norm_gain, expert_ids, route_probs, route_order, gate_weight, up_weight, down_weight):
    attended = attend(queries, new_keys, new_values, cache_keys, cache_values, cache_lengths)
    attention = jnp.dot(attended, out_weight, preferred_element_type=jnp.float32)
    residual = hidden_in.astype(jnp.float32) + attention
    normed = apply_norm(residual, norm_gain)
    blocks = SEQS // SEQ_DEV
    tables = jax.vmap(partial(route_tables, experts=EXPERTS, capacity=CAP))
    select_experts, weighted_output = tables(expert_ids.reshape(blocks, SEQ_DEV, TOP), route_probs.reshape(blocks, SEQ_DEV, TOP), route_order.reshape(blocks, SEQ_DEV, TOP))
    block_row_count = normed.astype(jnp.float32).reshape(blocks, SEQ_DEV, D)
    token_rows = jnp.einsum('cgh,cga->cha', select_experts, block_row_count, precision=lax.Precision.HIGHEST).astype(jnp.bfloat16)
    token_rows = token_rows.reshape(blocks, EXPERTS, CAP, D).transpose(1, 0, 2, 3).reshape(EXPERTS, blocks * CAP, D)
    expert_output = lax.map(expert_block, (token_rows, gate_weight, up_weight, down_weight))
    expert_output = expert_output.reshape(EXPERTS, blocks, CAP, D).transpose(1, 0, 2, 3).reshape(blocks, EXPERTS * CAP, D)
    expert_mixture = jnp.einsum('nyz,nzs->nys', weighted_output, expert_output, precision=lax.Precision.HIGHEST)
    return (residual + expert_mixture.reshape(SEQS, D)).astype(jnp.bfloat16)
```

```python
import functools

import jax
import jax.numpy as jnp
from jax import lax
from jax.experimental import pallas as pl
from jax.experimental.pallas import tpu as pltpu
from jax.sharding import PartitionSpec as P

EPSILON = 1e-05
GLU_SLOPE = 1.702
MESH = pl.DeviceIdType.MESH
BF16 = jnp.bfloat16
F32 = jnp.float32
CHUNK = 1024


def dot(a, b):
    return jnp.dot(a, b, preferred_element_type=F32)


def dot_nt(a, b):
    return lax.dot_general(a, b, (((1,), (1,)), ((), ())), preferred_element_type=F32)


def dot_tn(a, b):
    return lax.dot_general(a, b, (((0,), (0,)), ((), ())), preferred_element_type=F32)


def widths_of(total):
    out = []
    start = 0
    while start < total:
        out.append((start, min(CHUNK, total - start)))
        start += CHUNK
    return out


def kernel(
    sizes,
    len_ref,
    hid_ref,
    q_ref,
    nk_ref,
    nv_ref,
    gain_ref,
    ids_ref,
    probs_ref,
    order_ref,
    k_hbm,
    v_hbm,
    w_hbm,
    gate_hbm,
    up_hbm,
    down_hbm,
    out_ref,
    kbuf,
    vbuf,
    wbuf,
    gbuf,
    ubuf,
    dbuf,
    res_slab,
    disp_send,
    disp_recv,
    part_send,
    part_recv,
    ret_send,
    ret_recv,
    local_sem,
    xs_sem,
    xr_sem,
    ds_sem,
    dr_sem,
    ps_sem,
    pr_sem,
    rs_sem,
    rr_sem,
    *x_bufs,
):
    S, H, G, HD, C, D, F, E, T, cap = sizes
    R = H // G
    slab = D // T
    chunks = widths_of(D)
    x_send, x_recv = x_bufs[: len(chunks)], x_bufs[len(chunks) :]
    me_e = lax.axis_index("expert")
    me_t = lax.axis_index("tensor")

    copies = []
    for n, (src, dst) in enumerate(
        (
            (k_hbm, kbuf),
            (v_hbm, vbuf),
            (w_hbm, wbuf),
            (gate_hbm.at[0], gbuf),
            (up_hbm.at[0], ubuf),
            (down_hbm.at[0], dbuf),
        )
    ):
        copies.append(pltpu.make_async_copy(src, dst, local_sem.at[n]))
    for copy in copies:
        copy.start()

    barrier = pltpu.get_barrier_semaphore()
    tensor_peers = [lax.rem(me_t + i, T) for i in range(1, T)]
    expert_peers = [lax.rem(me_e + i, E) for i in range(1, E)]
    for peer in tensor_peers:
        pl.semaphore_signal(barrier, inc=1, device_id={"tensor": peer}, device_id_type=MESH)
    for peer in expert_peers:
        pl.semaphore_signal(barrier, inc=1, device_id={"expert": peer}, device_id_type=MESH)

    ids = ids_ref[...]
    probs = probs_ref[...]
    order = order_ref[...]
    top = ids.shape[0]
    slots = E * cap
    row = lax.broadcasted_iota(jnp.int32, (slots, S), 0)
    slot_expert = row // cap
    slot_place = (row % cap).astype(F32)
    picked = jnp.zeros((top, S), F32)
    for j in range(top):
        picked = picked + jnp.where(order == j, probs[j : j + 1], 0.0)
    weights = picked / jnp.sum(probs, axis=0, keepdims=True)
    member = jnp.zeros((slots, S), F32)
    mixture = jnp.zeros((slots, S), F32)
    for j in range(top):
        hit = ids[j : j + 1] == slot_expert
        member = member + jnp.where(hit, 1.0, 0.0)
        mixture = mixture + jnp.where(hit, weights[j : j + 1], 0.0)
    earlier = jnp.where(
        lax.broadcasted_iota(jnp.int32, (S, S), 0) < lax.broadcasted_iota(jnp.int32, (S, S), 1),
        1.0,
        0.0,
    )
    place = dot(member.astype(BF16), earlier.astype(BF16))
    sel = jnp.where(place == slot_place, member, 0.0)
    mixture = mixture * sel
    mix_hi = mixture.astype(BF16)
    rest = mixture - mix_hi.astype(F32)
    mix_mid = rest.astype(BF16)
    mix_lo = (rest - mix_mid.astype(F32)).astype(BF16)

    scaling = 1.0 / HD**0.5
    width = G * HD
    diagonal = (lax.broadcasted_iota(jnp.int32, (H, width), 0) // R) == (
        lax.broadcasted_iota(jnp.int32, (H, width), 1) // HD
    )
    position = lax.broadcasted_iota(jnp.int32, (H, C), 1)
    copies[0].wait()
    scores, owns = [], []
    for s in range(S):
        wide = jnp.concatenate([q_ref[s].astype(F32)] * G, axis=1)
        wide = jnp.where(diagonal, wide, 0.0)
        raw = dot(wide.astype(BF16), kbuf[s].reshape(width, C)) * scaling
        scores.append(jnp.where(position < len_ref[s], raw, -1e30))
        new_key = nk_ref[s].astype(F32)
        row = jnp.concatenate([new_key[g : g + 1] for g in range(G)], axis=1)
        owns.append(jnp.sum(wide * row, axis=1, keepdims=True) * scaling)
    score = jnp.concatenate(scores, axis=0)
    own = jnp.concatenate(owns, axis=0)
    highest = jnp.maximum(jnp.max(score, axis=1, keepdims=True), own)
    grown = jnp.exp(score - highest)
    own_grown = jnp.exp(own - highest)
    total = jnp.sum(grown, axis=1, keepdims=True) + own_grown
    prob = (grown / total).astype(BF16)
    own_prob = (own_grown / total).astype(BF16).astype(F32)
    copies[1].wait()
    attended = []
    for s in range(S):
        rows = slice(s * H, (s + 1) * H)
        mixed = dot_nt(prob[rows], vbuf[s].reshape(width, C))
        new_value = nv_ref[s].astype(F32)
        row = jnp.concatenate([new_value[g : g + 1] for g in range(G)], axis=1)
        attended.append(jnp.where(diagonal, mixed + own_prob[rows] * row, 0.0))
    attended = jnp.concatenate(attended, axis=0).astype(BF16)
    out_row = lax.broadcasted_iota(jnp.int32, (R * S, S * H), 0)
    in_row = lax.broadcasted_iota(jnp.int32, (R * S, S * H), 1)
    regroup = jnp.where(
        ((out_row % S) == (in_row // H)) & ((out_row // S) == (in_row % R)), 1.0, 0.0
    ).astype(BF16)
    grouped = dot(regroup, attended)
    heads = jnp.concatenate(
        [
            grouped[r * S : (r + 1) * S, g * HD : (g + 1) * HD]
            for g in range(G)
            for r in range(R)
        ],
        axis=1,
    ).astype(BF16)

    pl.semaphore_wait(barrier, (T - 1) + (E - 1))
    copies[2].wait()
    partials, x_copies = [], []
    for c, (start, size) in enumerate(chunks):
        partial = dot_nt(heads, wbuf[start : start + size])
        partials.append(partial)
        x_send[c][...] = partial.astype(BF16)
        for i, peer in enumerate(tensor_peers):
            copy = pltpu.make_async_remote_copy(
                src_ref=x_send[c],
                dst_ref=x_recv[c].at[i],
                send_sem=xs_sem.at[c, i],
                recv_sem=xr_sem.at[c, i],
                device_id={"tensor": peer},
                device_id_type=MESH,
            )
            copy.start()
            x_copies.append((c, i, copy))
    residuals = [hid_ref[:, a : a + n].astype(F32) + partials[c] for c, (a, n) in enumerate(chunks)]
    for c, i, copy in x_copies:
        copy.wait()
        residuals[c] = residuals[c] + x_recv[c][i].astype(F32)
    residual = jnp.concatenate(residuals, axis=1)
    mean_square = jnp.sum(residual * residual, axis=1, keepdims=True) * (1.0 / D)
    normed = (residual * lax.rsqrt(mean_square + EPSILON) * gain_ref[...].reshape(1, D)).astype(BF16)
    for t in range(T):
        res_slab[t] = residual[:, t * slab : (t + 1) * slab]

    outgoing = dot(sel.astype(BF16), normed)
    for e in range(E):
        disp_send[e] = outgoing[e * cap : (e + 1) * cap].astype(BF16)
    d_copies = []
    for i, peer in enumerate(expert_peers):
        copy = pltpu.make_async_remote_copy(
            src_ref=disp_send.at[peer],
            dst_ref=disp_recv.at[me_e],
            send_sem=ds_sem.at[i],
            recv_sem=dr_sem.at[i],
            device_id={"expert": peer},
            device_id_type=MESH,
        )
        copy.start()
        d_copies.append(copy)
    disp_recv[me_e] = disp_send[me_e]
    copies[3].wait()
    copies[4].wait()
    copies[5].wait()
    for copy in d_copies:
        copy.wait()
    arrived = jnp.concatenate([disp_recv[e].astype(F32) for e in range(E)], axis=0).astype(BF16)

    gate = dot_nt(arrived, gbuf[...])
    upward = dot_nt(arrived, ubuf[...])
    active = (gate * jax.nn.sigmoid(GLU_SLOPE * gate) * (upward + 1.0)).astype(BF16)
    expert_part = dot(active, dbuf[...])

    for t in range(T):
        part_send[t] = expert_part[:, t * slab : (t + 1) * slab].astype(BF16)
    p_copies = []
    for i, peer in enumerate(tensor_peers):
        copy = pltpu.make_async_remote_copy(
            src_ref=part_send.at[peer],
            dst_ref=part_recv.at[i],
            send_sem=ps_sem.at[i],
            recv_sem=pr_sem.at[i],
            device_id={"tensor": peer},
            device_id_type=MESH,
        )
        copy.start()
        p_copies.append(copy)
    summed = part_send[me_t].astype(F32)
    for i, copy in enumerate(p_copies):
        copy.wait()
        summed = summed + part_recv[i].astype(F32)

    for e in range(E):
        ret_send[e] = summed[e * cap : (e + 1) * cap].astype(BF16)
    r_copies = []
    for i, peer in enumerate(expert_peers):
        copy = pltpu.make_async_remote_copy(
            src_ref=ret_send.at[peer],
            dst_ref=ret_recv.at[me_e],
            send_sem=rs_sem.at[i],
            recv_sem=rr_sem.at[i],
            device_id={"expert": peer},
            device_id_type=MESH,
        )
        copy.start()
        r_copies.append(copy)
    ret_recv[me_e] = ret_send[me_e]
    kept = res_slab[me_t]
    for copy in r_copies:
        copy.wait()
    returned = jnp.concatenate([ret_recv[e].astype(F32) for e in range(E)], axis=0).astype(BF16)
    blended = dot_tn(mix_hi, returned) + (dot_tn(mix_mid, returned) + dot_tn(mix_lo, returned))
    out_ref[...] = (kept + blended).astype(BF16)


def per_device(
    hidden_in,
    queries,
    new_keys,
    new_values,
    cache_keys,
    cache_values,
    cache_lengths,
    out_weight,
    norm_gain,
    expert_ids,
    route_probs,
    route_order,
    gate_weight,
    up_weight,
    down_weight,
):
    S, D = hidden_in.shape
    E = lax.axis_size("expert")
    T = lax.axis_size("tensor")
    assert gate_weight.shape[0] == 1
    H, HD = queries.shape[1:]
    G = new_keys.shape[1]
    C = cache_keys.shape[3]
    F = gate_weight.shape[2]
    top = expert_ids.shape[1]
    cap = min(S, max(2, (S * top + E - 1) // E))
    slab = D // T
    chunks = widths_of(D)
    sizes = (S, H, G, HD, C, D, F, E, T, cap)
    vmem = pl.BlockSpec(memory_space=pltpu.VMEM)
    hbm = pl.BlockSpec(memory_space=pl.ANY)
    smem = pl.BlockSpec(memory_space=pltpu.SMEM)
    scratch = [
        pltpu.VMEM(cache_keys.shape, BF16),
        pltpu.VMEM(cache_values.shape, BF16),
        pltpu.VMEM((D, H * HD), BF16),
        pltpu.VMEM((F, D), BF16),
        pltpu.VMEM((F, D), BF16),
        pltpu.VMEM((F, D), BF16),
        pltpu.VMEM((T, S, slab), F32),
        pltpu.VMEM((E, cap, D), BF16),
        pltpu.VMEM((E, cap, D), BF16),
        pltpu.VMEM((T, E * cap, slab), BF16),
        pltpu.VMEM((T - 1, E * cap, slab), BF16),
        pltpu.VMEM((E, cap, slab), BF16),
        pltpu.VMEM((E, cap, slab), BF16),
        pltpu.SemaphoreType.DMA((6,)),
        pltpu.SemaphoreType.DMA((len(chunks), T - 1)),
        pltpu.SemaphoreType.DMA((len(chunks), T - 1)),
        pltpu.SemaphoreType.DMA((E - 1,)),
        pltpu.SemaphoreType.DMA((E - 1,)),
        pltpu.SemaphoreType.DMA((T - 1,)),
        pltpu.SemaphoreType.DMA((T - 1,)),
        pltpu.SemaphoreType.DMA((E - 1,)),
        pltpu.SemaphoreType.DMA((E - 1,)),
    ]
    scratch += [pltpu.VMEM((S, n), BF16) for _, n in chunks]
    scratch += [pltpu.VMEM((T - 1, S, n), BF16) for _, n in chunks]
    return pl.pallas_call(
        functools.partial(kernel, sizes),
        out_shape=jax.ShapeDtypeStruct((S, slab), BF16),
        in_specs=[smem] + [vmem] * 8 + [hbm] * 6,
        out_specs=vmem,
        scratch_shapes=scratch,
        compiler_params=pltpu.CompilerParams(
            collective_id=0, has_side_effects=True, vmem_limit_bytes=60 * 1024 * 1024
        ),
    )(
        cache_lengths,
        hidden_in,
        queries,
        new_keys,
        new_values,
        norm_gain,
        expert_ids.T,
        route_probs.T,
        route_order.T,
        cache_keys,
        cache_values,
        out_weight.T,
        gate_weight.transpose(0, 2, 1),
        up_weight.transpose(0, 2, 1),
        down_weight,
    )


def solution(mesh):
    in_specs = (
        P(("groups", "expert"), None),
        P(("groups", "expert"), "tensor", None),
        P(("groups", "expert"), "tensor", None),
        P(("groups", "expert"), "tensor", None),
        P(("groups", "expert"), "tensor", None, None),
        P(("groups", "expert"), "tensor", None, None),
        P(("groups", "expert")),
        P("tensor", None),
        P(),
        P(("groups", "expert"), None),
        P(("groups", "expert"), None),
        P(("groups", "expert"), None),
        P("expert", None, "tensor"),
        P("expert", None, "tensor"),
        P("expert", "tensor", None),
    )
    out_specs = P(("groups", "expert"), "tensor")
    return jax.shard_map(
        per_device, mesh=mesh, in_specs=in_specs, out_specs=out_specs, check_vma=False
    )
```

```python
import functools

import jax
import jax.numpy as jnp
from jax import lax
from jax.experimental import pallas as pl
from jax.experimental.pallas import tpu as pltpu
from jax.sharding import PartitionSpec as P

EPSILON = 1e-05
GLU_SLOPE = 1.702
MESH = pl.DeviceIdType.MESH
BF16 = jnp.bfloat16
F32 = jnp.float32
CHUNK = 1024
PART = 1536
LANES = 128


def dot(a, b):
    return jnp.dot(a, b, preferred_element_type=F32)


def dot_nt(a, b):
    return lax.dot_general(a, b, (((1,), (1,)), ((), ())), preferred_element_type=F32)


def dot_tn(a, b):
    return lax.dot_general(a, b, (((0,), (0,)), ((), ())), preferred_element_type=F32)


def widths_of(total, step):
    return [(start, min(step, total - start)) for start in range(0, total, step)]


def split_three(x):
    high = x.astype(BF16)
    rest = x - high.astype(F32)
    middle = rest.astype(BF16)
    low = (rest - middle.astype(F32)).astype(BF16)
    return high, middle, low


def kernel(
    sizes,
    len_ref,
    hid_ref,
    q_ref,
    nk_ref,
    nv_ref,
    gain_ref,
    ids_ref,
    probs_ref,
    order_ref,
    k_hbm,
    v_hbm,
    w_hbm,
    gate_hbm,
    up_hbm,
    down_hbm,
    out_ref,
    kbuf,
    vbuf,
    wbuf,
    gbuf,
    ubuf,
    dbuf,
    res_slab,
    local_sem,
    weight_sem,
    xs_sem,
    xr_sem,
    ds_sem,
    dr_sem,
    rs_sem,
    rr_sem,
    *bufs,
):
    S, H, G, HD, C, D, F, E, T, cap = sizes
    R = H // G
    slab = D // T
    chunks = widths_of(D, CHUNK)
    parts = widths_of(slab, PART)
    groups = []
    taken = 0
    for count in [len(chunks)] * 4 + [len(parts)] * 2:
        groups.append(bufs[taken : taken + count])
        taken += count
    x_send, x_recv, disp_send, disp_recv, ret_send, ret_recv = groups
    me_e = lax.axis_index("expert")
    me_t = lax.axis_index("tensor")

    k_copy = pltpu.make_async_copy(k_hbm, kbuf, local_sem.at[0])
    v_copy = pltpu.make_async_copy(v_hbm, vbuf, local_sem.at[1])
    w_copies = [
        pltpu.make_async_copy(w_hbm.at[pl.ds(a, n)], wbuf.at[pl.ds(a, n)], weight_sem.at[c])
        for c, (a, n) in enumerate(chunks)
    ]
    gate_copy = pltpu.make_async_copy(gate_hbm.at[0], gbuf, local_sem.at[2])
    up_copy = pltpu.make_async_copy(up_hbm.at[0], ubuf, local_sem.at[3])
    down_copy = pltpu.make_async_copy(down_hbm.at[0], dbuf, local_sem.at[4])
    k_copy.start()
    v_copy.start()
    for copy in w_copies:
        copy.start()

    barrier = pltpu.get_barrier_semaphore()
    tensor_peers = [lax.rem(me_t + i, T) for i in range(1, T)]
    expert_peers = [lax.rem(me_e + i, E) for i in range(1, E)]
    peers = [
        {"expert": lax.rem(me_e + i, E), "tensor": lax.rem(me_t + j, T)}
        for i in range(E)
        for j in range(T)
        if i + j > 0
    ]
    for peer in peers:
        pl.semaphore_signal(barrier, inc=1, device_id=peer, device_id_type=MESH)

    ids = ids_ref[...]
    probs = probs_ref[...]
    order = order_ref[...]
    top = ids.shape[0]
    slots = E * cap
    row = lax.broadcasted_iota(jnp.int32, (slots, S), 0)
    slot_expert = row // cap
    slot_place = (row % cap).astype(F32)
    picked = jnp.zeros((top, S), F32)
    for j in range(top):
        picked = picked + jnp.where(order == j, probs[j : j + 1], 0.0)
    weights = picked / jnp.sum(probs, axis=0, keepdims=True)
    member = jnp.zeros((slots, S), F32)
    mixture = jnp.zeros((slots, S), F32)
    for j in range(top):
        hit = ids[j : j + 1] == slot_expert
        member = member + jnp.where(hit, 1.0, 0.0)
        mixture = mixture + jnp.where(hit, weights[j : j + 1], 0.0)
    earlier = jnp.where(
        lax.broadcasted_iota(jnp.int32, (S, S), 0) < lax.broadcasted_iota(jnp.int32, (S, S), 1),
        1.0,
        0.0,
    )
    place = dot(member.astype(BF16), earlier.astype(BF16))
    sel = jnp.where(place == slot_place, member, 0.0)
    mixture = mixture * sel
    mixture = split_three(mixture)
    sel = sel.astype(BF16)

    scaling = 1.0 / HD**0.5
    width = G * HD
    diagonal = (lax.broadcasted_iota(jnp.int32, (H, width), 0) // R) == (
        lax.broadcasted_iota(jnp.int32, (H, width), 1) // HD
    )
    position = lax.broadcasted_iota(jnp.int32, (H, C), 1)
    k_copy.wait()
    scores, owns = [], []
    for s in range(S):
        wide = jnp.concatenate([q_ref[s].astype(F32)] * G, axis=1)
        wide = jnp.where(diagonal, wide, 0.0)
        raw = dot(wide.astype(BF16), kbuf[s].reshape(width, C)) * scaling
        scores.append(jnp.where(position < len_ref[s], raw, -1e30))
        new_key = nk_ref[s].astype(F32)
        row = jnp.concatenate([new_key[g : g + 1] for g in range(G)], axis=1)
        owns.append(jnp.sum(wide * row, axis=1, keepdims=True) * scaling)
    score = jnp.concatenate(scores, axis=0)
    own = jnp.concatenate(owns, axis=0)
    highest = jnp.maximum(jnp.max(score, axis=1, keepdims=True), own)
    grown = jnp.exp(score - highest)
    own_grown = jnp.exp(own - highest)
    total = jnp.sum(grown, axis=1, keepdims=True) + own_grown
    prob = (grown / total).astype(BF16)
    own_prob = (own_grown / total).astype(BF16).astype(F32)
    v_copy.wait()
    attended = []
    for s in range(S):
        rows = slice(s * H, (s + 1) * H)
        mixed = dot_nt(prob[rows], vbuf[s].reshape(width, C))
        new_value = nv_ref[s].astype(F32)
        row = jnp.concatenate([new_value[g : g + 1] for g in range(G)], axis=1)
        attended.append(jnp.where(diagonal, mixed + own_prob[rows] * row, 0.0))
    attended = jnp.concatenate(attended, axis=0).astype(BF16)
    out_row = lax.broadcasted_iota(jnp.int32, (R * S, S * H), 0)
    in_row = lax.broadcasted_iota(jnp.int32, (R * S, S * H), 1)
    regroup = jnp.where(
        ((out_row % S) == (in_row // H)) & ((out_row // S) == (in_row % R)), 1.0, 0.0
    ).astype(BF16)
    grouped = dot(regroup, attended)
    heads = jnp.concatenate(
        [
            grouped[r * S : (r + 1) * S, g * HD : (g + 1) * HD]
            for g in range(G)
            for r in range(R)
        ],
        axis=1,
    ).astype(BF16)

    pl.semaphore_wait(barrier, len(peers))
    residuals, x_copies = [], []
    for c, (a, n) in enumerate(chunks):
        w_copies[c].wait()
        if c == len(chunks) - 1:
            gate_copy.start()
            up_copy.start()
            down_copy.start()
        partial = dot_nt(heads, wbuf[a : a + n])
        x_send[c][...] = partial.astype(BF16)
        x_copies.append([])
        for i, peer in enumerate(tensor_peers):
            copy = pltpu.make_async_remote_copy(
                src_ref=x_send[c],
                dst_ref=x_recv[c].at[i],
                send_sem=xs_sem.at[c, i],
                recv_sem=xr_sem.at[c, i],
                device_id={"tensor": peer},
                device_id_type=MESH,
            )
            copy.start()
            x_copies[c].append(copy)
        residuals.append(hid_ref[:, a : a + n].astype(F32) + partial)

    gain = gain_ref[...].reshape(1, D)
    square = jnp.zeros((S, 1), F32)
    d_copies = []
    for c, (a, n) in enumerate(chunks):
        for i, copy in enumerate(x_copies[c]):
            copy.wait()
            residuals[c] = residuals[c] + x_recv[c][i].astype(F32)
        square = square + jnp.sum(residuals[c] * residuals[c], axis=1, keepdims=True)
        rows = (residuals[c] * gain[:, a : a + n]).astype(BF16)
        if c == len(chunks) - 1:
            factor = lax.rsqrt(square * (1.0 / D) + EPSILON)
            lane = lax.broadcasted_iota(jnp.int32, (S, LANES), 1)
            extra = jnp.zeros((S, LANES), F32)
            for i, term in enumerate(split_three(factor)):
                extra = jnp.where(lane == i, term.astype(F32), extra)
            rows = jnp.concatenate([extra.astype(BF16), rows], axis=1)
        outgoing = dot(sel, rows)
        for e in range(E):
            disp_send[c][e] = outgoing[e * cap : (e + 1) * cap].astype(BF16)
        d_copies.append([])
        for i, peer in enumerate(expert_peers):
            copy = pltpu.make_async_remote_copy(
                src_ref=disp_send[c].at[peer],
                dst_ref=disp_recv[c].at[me_e],
                send_sem=ds_sem.at[c, i],
                recv_sem=dr_sem.at[c, i],
                device_id={"expert": peer},
                device_id_type=MESH,
            )
            copy.start()
            d_copies[c].append(copy)
        disp_recv[c][me_e] = disp_send[c][me_e]
    residual = jnp.concatenate(residuals, axis=1)
    for t in range(T):
        res_slab[t] = residual[:, t * slab : (t + 1) * slab]

    gate_copy.wait()
    up_copy.wait()
    gate = jnp.zeros((slots, F), F32)
    upward = jnp.zeros((slots, F), F32)
    for c, (a, n) in enumerate(chunks):
        for copy in d_copies[c]:
            copy.wait()
        arrived = jnp.concatenate([disp_recv[c][e].astype(F32) for e in range(E)], axis=0)
        if c == len(chunks) - 1:
            factor = jnp.sum(arrived[:, :LANES], axis=1, keepdims=True)
            arrived = arrived[:, LANES:]
        arrived = arrived.astype(BF16)
        gate = gate + dot_nt(arrived, gbuf[:, a : a + n])
        upward = upward + dot_nt(arrived, ubuf[:, a : a + n])
    gate = gate * factor
    upward = upward * factor
    active = (gate * jax.nn.sigmoid(GLU_SLOPE * gate) * (upward + 1.0)).astype(BF16)

    down_copy.wait()
    r_copies = []
    for c, (a, n) in enumerate(parts):
        for t in range(T):
            first = t * slab + a
            low = first // LANES * LANES
            high = min(D, -(-(first + n) // LANES) * LANES)
            product = dot(active, dbuf[:, low:high])[:, first - low : first - low + n]
            for e in range(E):
                ret_send[c][t, e] = product[e * cap : (e + 1) * cap].astype(BF16)
        r_copies.append([])
        for i, peer in enumerate(peers):
            copy = pltpu.make_async_remote_copy(
                src_ref=ret_send[c].at[peer["tensor"], peer["expert"]],
                dst_ref=ret_recv[c].at[me_t, me_e],
                send_sem=rs_sem.at[c, i],
                recv_sem=rr_sem.at[c, i],
                device_id=peer,
                device_id_type=MESH,
            )
            copy.start()
            r_copies[c].append(copy)
        ret_recv[c][me_t, me_e] = ret_send[c][me_t, me_e]

    kept = res_slab[me_t]
    for c, (a, n) in enumerate(parts):
        for copy in r_copies[c]:
            copy.wait()
        returned = jnp.zeros((slots, n), F32)
        for t in range(T):
            returned = returned + jnp.concatenate(
                [ret_recv[c][t, e].astype(F32) for e in range(E)], axis=0
            )
        high, middle, low = split_three(returned)
        blended = dot_tn(mixture[0], high)
        blended = blended + (dot_tn(mixture[1], high) + dot_tn(mixture[0], middle))
        blended = blended + (
            dot_tn(mixture[2], high) + dot_tn(mixture[1], middle) + dot_tn(mixture[0], low)
        )
        out_ref[:, a : a + n] = (kept[:, a : a + n] + blended).astype(BF16)


def per_device(
    hidden_in,
    queries,
    new_keys,
    new_values,
    cache_keys,
    cache_values,
    cache_lengths,
    out_weight,
    norm_gain,
    expert_ids,
    route_probs,
    route_order,
    gate_weight,
    up_weight,
    down_weight,
):
    S, D = hidden_in.shape
    E = lax.axis_size("expert")
    T = lax.axis_size("tensor")
    assert gate_weight.shape[0] == 1
    H, HD = queries.shape[1:]
    G = new_keys.shape[1]
    C = cache_keys.shape[3]
    F = gate_weight.shape[2]
    top = expert_ids.shape[1]
    cap = min(S, max(2, (S * top + E - 1) // E))
    slab = D // T
    chunks = widths_of(D, CHUNK)
    parts = widths_of(slab, PART)
    sizes = (S, H, G, HD, C, D, F, E, T, cap)
    vmem = pl.BlockSpec(memory_space=pltpu.VMEM)
    hbm = pl.BlockSpec(memory_space=pl.ANY)
    smem = pl.BlockSpec(memory_space=pltpu.SMEM)
    scratch = [
        pltpu.VMEM(cache_keys.shape, BF16),
        pltpu.VMEM(cache_values.shape, BF16),
        pltpu.VMEM((D, H * HD), BF16),
        pltpu.VMEM((F, D), BF16),
        pltpu.VMEM((F, D), BF16),
        pltpu.VMEM((F, D), BF16),
        pltpu.VMEM((T, S, slab), F32),
        pltpu.SemaphoreType.DMA((5,)),
        pltpu.SemaphoreType.DMA((len(chunks),)),
        pltpu.SemaphoreType.DMA((len(chunks), T - 1)),
        pltpu.SemaphoreType.DMA((len(chunks), T - 1)),
        pltpu.SemaphoreType.DMA((len(chunks), E - 1)),
        pltpu.SemaphoreType.DMA((len(chunks), E - 1)),
        pltpu.SemaphoreType.DMA((len(parts), T * E - 1)),
        pltpu.SemaphoreType.DMA((len(parts), T * E - 1)),
    ]
    wide = [n for _, n in chunks]
    sent = wide[:-1] + [wide[-1] + LANES]
    narrow = [n for _, n in parts]
    scratch += [pltpu.VMEM((S, n), BF16) for n in wide]
    scratch += [pltpu.VMEM((T - 1, S, n), BF16) for n in wide]
    scratch += [pltpu.VMEM((E, cap, n), BF16) for n in sent] * 2
    scratch += [pltpu.VMEM((T, E, cap, n), BF16) for n in narrow] * 2
    return pl.pallas_call(
        functools.partial(kernel, sizes),
        out_shape=jax.ShapeDtypeStruct((S, slab), BF16),
        in_specs=[smem] + [vmem] * 8 + [hbm] * 6,
        out_specs=vmem,
        scratch_shapes=scratch,
        compiler_params=pltpu.CompilerParams(
            collective_id=0, has_side_effects=True, vmem_limit_bytes=60 * 1024 * 1024
        ),
    )(
        cache_lengths,
        hidden_in,
        queries,
        new_keys,
        new_values,
        norm_gain,
        expert_ids.T,
        route_probs.T,
        route_order.T,
        cache_keys,
        cache_values,
        out_weight.T,
        gate_weight.transpose(0, 2, 1),
        up_weight.transpose(0, 2, 1),
        down_weight,
    )


def solution(mesh):
    in_specs = (
        P(("groups", "expert"), None),
        P(("groups", "expert"), "tensor", None),
        P(("groups", "expert"), "tensor", None),
        P(("groups", "expert"), "tensor", None),
        P(("groups", "expert"), "tensor", None, None),
        P(("groups", "expert"), "tensor", None, None),
        P(("groups", "expert")),
        P("tensor", None),
        P(),
        P(("groups", "expert"), None),
        P(("groups", "expert"), None),
        P(("groups", "expert"), None),
        P("expert", None, "tensor"),
        P("expert", None, "tensor"),
        P("expert", "tensor", None),
    )
    out_specs = P(("groups", "expert"), "tensor")
    return jax.shard_map(
        per_device, mesh=mesh, in_specs=in_specs, out_specs=out_specs, check_vma=False
    )
```
